32 devices in a mesh: aa: 4 (over x, core), ba: 8 (over z, y).
Axes of the slice: x: 2, y: 2, z: 4, core: 2. Of those that a mesh axis runs over, the one named last changes fastest.
Arguments:
- head_outputs: bfloat16 [1024, 4096], P('ba'), may hold values from -6 to 6
- stream: bfloat16 [1024, 4096], P('ba'), may hold values from -6 to 6
- adapter_down_factors: bfloat16 [4096, 512], P(None, 'aa'), may hold values from -0.09375 to 0.09375
- adapter_up_factors: bfloat16 [512, 4096], P('aa'), may hold values from -1.5 to 1.5
- norm_gain_vector: float32 [4096], replicated, may hold values from 0.5 to 1.5
- router_matrix: bfloat16 [4096, 8], replicated, may hold values from -0.09375 to 0.09375
- token_adapter_index: int32 [1024], P('ba'), may hold values from 0 to 31
- token_expert_index: int32 [1024, 2], P('ba'), may hold values from 0 to 7, all different within a row; in each aligned block of 128 rows (0 to 127, 128 to 255, ...) at most 48 rows name the same one
- gate_weight: bfloat16 [8, 4096, 14336], P('ba', None, 'aa'), may hold values from -0.09375 to 0.09375
- up_weight: bfloat16 [8, 4096, 14336], P('ba', None, 'aa'), may hold values from -0.09375 to 0.09375
- down_weight: bfloat16 [8, 14336, 4096], P('ba', 'aa'), may hold values from -0.046875 to 0.046875
Outputs:
- mixed: bfloat16 [1024, 4096], P('ba', 'aa')
- adapter_load: float32 [32], P('aa')
The draws below stay inside these ranges and needn't reach their ends.
Inputs may be any that keep to these rules, and one draw needn't show every extreme that they name: `token_expert_index`: the two experts of a row differ; in each aligned block of 128 rows no expert is named by more than 48 rows.
All inputs are finite; a program needn't handle non-finite values.
Results may differ from the reference program's by a relative error of at most 0.0049.
Values may be sent and summed in bfloat16 or wider, within the bound.
No kernel may reach another device: no remote copies, remote signals or barrier semaphores. Data moves between devices by JAX's collectives and lax.ppermute only.
A program may use at most 192 MiB of HBM per device.

```python
import math
import jax
import jax.numpy as jnp
import numpy as np
from jax import lax

MODEL_DIM = 4096
FF = 14336
E = 8
ADAPTER_RANK = 16
TOK_DEV = 128
CAP = 48
TOKENS = 1024
ADAPTER_COUNT = 32
SLOTS = 8
SLOT_FF = 14336
N_BA = 8


def plant(drawn, stream_key, smallest, top_value):
    longest = drawn.shape.index(max(drawn.shape))
    spots = []
    for shift in (0, 1):
        where = [jax.random.randint(jax.random.fold_in(stream_key, axis), (), 0, length) for axis, length in enumerate(drawn.shape)]
        where[longest] = (where[longest] + shift) % drawn.shape[longest]
        spots.append(tuple(where))
    return drawn.at[spots[0]].set(smallest).at[spots[1]].set(top_value)


def shard_levels(rng, shape, split, smallest, high):
    factor_of = 1.0
    for dim, shards_of in split:
        heights = jax.random.uniform(jax.random.fold_in(jax.random.fold_in(rng, 6), dim), (shards_of,), jnp.float32, smallest / len(split), high / len(split))
        factor_of = factor_of * jnp.repeat(jnp.exp(heights), shape[dim] // shards_of).reshape((-1,) + (1,) * (len(shape) - 1 - dim))
    return factor_of


def rank_bounds(count, lean):
    loads = [(1 << 20) // math.isqrt(rank ** lean) + 1 for rank in range(1, count + 1)]
    deviation = 1 + sum(loads) // (1 << 30)
    return np.cumsum(np.array([max(1, weight // deviation) for weight in loads]))


def skewed_ids(own_key, extent, amount, slope):
    table = rank_bounds(amount, slope)
    lot = jax.random.randint(jax.random.fold_in(own_key, 1), extent, 0, int(table[amount - 1]))
    rank = jnp.searchsorted(jnp.asarray(table, jnp.int32), lot, side="right")
    return jax.random.permutation(jax.random.fold_in(own_key, 2), amount)[rank].astype(jnp.int32)


def deal_out(stream_key, own, number, rows, count, top, most, skew):
    sequence = jax.random.permutation(stream_key, count)
    heavy_load, ordinary = portions_of(count, rows * top, most, skew, True), portions_of(count, rows * top, most, skew, False)
    places = jnp.arange(count)

    def named(lengths, turn):
        used = int((lengths > 0).sum())
        fixed = max(1, used // 4)
        shifted = fixed + (places - fixed + turn * (used - fixed)) % max(1, count - fixed)
        return jnp.zeros((count,), jnp.int32).at[sequence[jnp.where(places < fixed, places, shifted)]].set(jnp.asarray(lengths, jnp.int32))

    lengths = jnp.where(number % 4 == 0, named(heavy_load, number // 4), named(ordinary, number - number // 4 - 1))
    mixed = jax.random.permutation(jax.random.fold_in(own, 3), count)
    giver, taker = mixed[0:count // 2 * 2:2], mixed[1:count // 2 * 2:2]
    margin = jnp.minimum(lengths[giver] - 1, most - lengths[taker]) // 2
    margin = jnp.where((giver == sequence[0]) | (taker == sequence[0]) | (lengths[taker] == 0), 0, jnp.maximum(margin, 0))
    shifted = jax.random.randint(jax.random.fold_in(own, 4), (count // 2,), 0, 1 << 20) % (margin + 1)
    lengths = lengths.at[giver].add(-shifted).at[taker].add(shifted)
    labels = jnp.searchsorted(jnp.cumsum(lengths), jnp.arange(rows * top), side="right").astype(jnp.int32)
    table = labels.reshape(top, rows).T
    table = table[jax.random.permutation(jax.random.fold_in(own, 1), rows)]
    turn = jax.random.randint(jax.random.fold_in(own, 2), (rows, 1), 0, top)
    return jnp.take_along_axis(table, (jnp.arange(top)[None, :] + turn) % top, axis=1)


def portions_of(amount, total, most, slope, full):
    portions = [(1 << 20) // math.isqrt(rank ** slope) + 1 for rank in range(1, amount + 1)]
    largest = most if full else min(most, max(-(-total // amount), total * portions[0] // sum(portions)))
    least = 1 if total - largest >= amount - 1 else 0
    counts, spare = [largest] + [least] * (amount - 1), total - largest - least * (amount - 1)
    while spare > 0:
        candidates = [i for i in range(1, amount) if counts[i] < largest] or [i for i in range(1, amount) if counts[i] < most]
        mass, remaining = sum([portions[i] for i in candidates]), spare
        for i in candidates:
            more = min(most - counts[i], max(1, remaining * portions[i] // mass), spare)
            counts[i] = counts[i] + more
            spare = spare - more
    return np.array(counts)


def bell_draw(key, extent, deviation, limit, shards=(), kind=jnp.bfloat16):
    values = jax.random.normal(key, extent, jnp.float32) * deviation
    if len(shards) > 0:
        values = shard_levels(key, extent, shards, -0.22, 0.18) * values
    return jnp.clip(values, min=-limit, max=limit).astype(kind)


def setup_inputs(seed: int = 0) -> dict:
    key_list = jax.random.split(jax.random.key(seed), 12)
    head_outputs = bell_draw(key_list[0], (TOKENS, MODEL_DIM), 1.0, 6.0, ((0, 8),))
    stream = bell_draw(key_list[1], (TOKENS, MODEL_DIM), 1.0, 6.0, ((0, 8),))
    adapter_down_factors = bell_draw(key_list[2], (MODEL_DIM, ADAPTER_COUNT * ADAPTER_RANK), MODEL_DIM ** -0.5, 0.09375, ((1, 4),))
    adapter_up_factors = bell_draw(key_list[3], (ADAPTER_COUNT * ADAPTER_RANK, MODEL_DIM), ADAPTER_RANK ** -0.5, 1.5, ((0, 4),))
    norm_gain_vector = jnp.clip(1.0 + 0.1 * jax.random.normal(key_list[4], (MODEL_DIM,), jnp.float32), 0.5, 1.5)
    router_matrix = bell_draw(key_list[5], (MODEL_DIM, E), MODEL_DIM ** -0.5, 0.09375)
    token_adapter_index = plant(skewed_ids(key_list[6], (TOKENS,), ADAPTER_COUNT, 2), jax.random.fold_in(key_list[6], 3), 0, ADAPTER_COUNT - 1).astype(jnp.int32)
    token_expert_index_keys = jax.random.split(jax.random.fold_in(key_list[7], 1), TOKENS // TOK_DEV)
    token_expert_index_turns = jax.random.permutation(jax.random.fold_in(key_list[7], 3), TOKENS // TOK_DEV)
    token_expert_index = jax.vmap(lambda own, number: deal_out(jax.random.fold_in(key_list[7], 2), own, number, TOK_DEV, E, 2, CAP, 2))(token_expert_index_keys, token_expert_index_turns).reshape((TOKENS, 2))
    gate_weight = bell_draw(key_list[8], (SLOTS, MODEL_DIM, SLOT_FF), MODEL_DIM ** -0.5, 0.09375, ((0, 8), (2, 4)))
    up_weight = bell_draw(key_list[9], (SLOTS, MODEL_DIM, SLOT_FF), MODEL_DIM ** -0.5, 0.09375, ((0, 8), (2, 4)))
    down_weight = bell_draw(key_list[10], (SLOTS, SLOT_FF, MODEL_DIM), FF ** -0.5, 0.046875, ((0, 8), (1, 4)))
    return dict(head_outputs=head_outputs, stream=stream, adapter_down_factors=adapter_down_factors, adapter_up_factors=adapter_up_factors, norm_gain_vector=norm_gain_vector, router_matrix=router_matrix, token_adapter_index=token_adapter_index, token_expert_index=token_expert_index, gate_weight=gate_weight, up_weight=up_weight, down_weight=down_weight)


EPS = 1e-05
ADAPTER_SCALE = 2.0

def reference(head_outputs, stream, adapter_down_factors, adapter_up_factors, norm_gain_vector, router_matrix, token_adapter_index, token_expert_index, gate_weight, up_weight, down_weight):
    rank_projected = jnp.dot(head_outputs, adapter_down_factors, preferred_element_type=jnp.float32)
    column_holder = jnp.arange(adapter_down_factors.shape[1], dtype=jnp.int32) // ADAPTER_RANK
    rank_projected = jnp.where(token_adapter_index[:, None] == column_holder[None, :], rank_projected, 0.0).astype(jnp.bfloat16)
    adapter_update = ADAPTER_SCALE * jnp.dot(rank_projected, adapter_up_factors, preferred_element_type=jnp.float32)
    residual_stream = stream.astype(jnp.float32) + adapter_update
    inv_norm = lax.rsqrt(lax.optimization_barrier(jnp.mean(residual_stream * residual_stream, axis=1, keepdims=True)) + EPS)
    normed = (residual_stream * inv_norm * norm_gain_vector).astype(jnp.bfloat16)
    logits = jnp.dot(normed, router_matrix, preferred_element_type=jnp.float32)
    picked = jnp.take_along_axis(logits, token_expert_index, axis=1)
    weights = 1.0 / (1.0 + jnp.exp(picked[:, ::-1] - picked))
    blocked = token_expert_index.reshape(N_BA, TOK_DEV * 2)
    expert_hits = (blocked[:, :, None] == jnp.arange(E, dtype=jnp.int32)[None, None, :]).astype(jnp.int32)
    before = jnp.cumsum(expert_hits, axis=1) - expert_hits
    position = lax.optimization_barrier(jnp.sum(before * expert_hits, axis=2))
    slot_index = (jnp.arange(N_BA, dtype=jnp.int32)[:, None] * CAP + position).reshape(-1)
    flat_experts = token_expert_index.reshape(-1)
    token_of = jnp.arange(TOKENS * 2, dtype=jnp.int32) // 2
    owner_tok = jnp.zeros((E, N_BA * CAP), jnp.int32).at[flat_experts, slot_index].set(token_of)
    halves = N_BA // E
    results = jnp.zeros((E, N_BA * CAP, normed.shape[1]), jnp.float32)
    for slot_number in range(N_BA):
        expert = slot_number // halves
        slot_rows = normed[owner_tok[expert]]
        gate_proj = jnp.dot(slot_rows, gate_weight[slot_number], preferred_element_type=jnp.float32)
        up_proj = jnp.dot(slot_rows, up_weight[slot_number], preferred_element_type=jnp.float32)
        hidden = (jax.nn.silu(gate_proj) * up_proj).astype(jnp.bfloat16)
        results = results.at[expert].add(jnp.dot(hidden, down_weight[slot_number], preferred_element_type=jnp.float32))
    expert_out = results[flat_experts, slot_index].reshape(TOKENS, 2, -1)
    mixed = residual_stream + lax.optimization_barrier(jnp.sum(weights[:, :, None] * expert_out, axis=1))
    adapter_load = lax.optimization_barrier(jnp.sum((token_adapter_index[:, None] == jnp.arange(ADAPTER_COUNT, dtype=jnp.int32)[None, :]).astype(jnp.float32), axis=0))
    return (mixed.astype(jnp.bfloat16), adapter_load)
```

```python
import functools

import jax
import jax.numpy as jnp
from jax import lax
from jax.experimental import pallas as pl
from jax.experimental.pallas import tpu as pltpu
from jax.sharding import PartitionSpec as P

ADAPTER_RANK = 16
CAP = 48

EPS = 1e-05
ADAPTER_SCALE = 2.0
COLUMN_CHUNKS = 2


def swap(value, axis, distance):
    size = lax.axis_size(axis)
    return lax.ppermute(value, axis, [(k, k ^ distance) for k in range(size)])


def tile_of(width, most):
    tile = most
    while width % tile:
        tile //= 2
    return tile


def gate_up_kernel(offset_ref, *refs, pieces, rows_of):
    piece_refs = refs[:pieces]
    gate_ref, up_ref, hidden_ref, x_ref, sem = refs[pieces:]

    @pl.when(pl.program_id(0) == 0)
    def _():
        copies = []
        for number, piece in enumerate(piece_refs):
            first, index = rows_of[number]
            count, width = piece.shape
            start = pl.multiple_of(offset_ref[index] * width, 128)
            copies.append(
                pltpu.make_async_copy(
                    piece,
                    x_ref.at[pl.ds(first, count), pl.ds(start, width)],
                    sem.at[number],
                )
            )
        for copy in copies:
            copy.start()
        for copy in copies:
            copy.wait()

    rows = x_ref[...]
    gate = jnp.dot(rows, gate_ref[...], preferred_element_type=jnp.float32)
    up = jnp.dot(rows, up_ref[...], preferred_element_type=jnp.float32)
    hidden_ref[...] = (gate / (1.0 + jnp.exp(-gate)) * up).astype(jnp.bfloat16)


def gate_up(pieces, rows_of, offsets, gate_weight, up_weight, total_rows):
    model_width, hidden_width = gate_weight.shape[1:]
    tile = tile_of(hidden_width, 512)
    count = len(pieces)
    weight_spec = pl.BlockSpec((None, model_width, tile), lambda n, s: (0, 0, n))
    return pl.pallas_call(
        functools.partial(gate_up_kernel, pieces=count, rows_of=rows_of),
        out_shape=jax.ShapeDtypeStruct((total_rows, hidden_width), jnp.bfloat16),
        grid_spec=pltpu.PrefetchScalarGridSpec(
            num_scalar_prefetch=1,
            grid=(hidden_width // tile,),
            in_specs=[pl.BlockSpec(memory_space=pl.ANY)] * count + [weight_spec, weight_spec],
            out_specs=pl.BlockSpec((total_rows, tile), lambda n, s: (0, n)),
            scratch_shapes=[
                pltpu.VMEM((total_rows, model_width), jnp.bfloat16),
                pltpu.SemaphoreType.DMA((count,)),
            ],
        ),
        compiler_params=pltpu.CompilerParams(
            dimension_semantics=("arbitrary",), vmem_limit_bytes=48 << 20
        ),
        name="gate_up",
    )(offsets, *pieces, gate_weight, up_weight)


def down_kernel(offset_ref, hidden_ref, down_ref, send_ref, keep_ref, *, sends):
    step = pl.program_id(0)
    part = jnp.dot(hidden_ref[...], down_ref[...], preferred_element_type=jnp.float32)

    @pl.when(step < sends)
    def _():
        send_ref[...] = part.astype(jnp.bfloat16)

    @pl.when(step >= sends)
    def _():
        keep_ref[...] = part


def down(hidden, blocks, down_weight, width, sends):
    total_rows, hidden_width = hidden.shape
    steps = blocks.shape[0]
    return pl.pallas_call(
        functools.partial(down_kernel, sends=sends),
        out_shape=(
            jax.ShapeDtypeStruct((sends, total_rows, width), jnp.bfloat16),
            jax.ShapeDtypeStruct((steps - sends, total_rows, width), jnp.float32),
        ),
        grid_spec=pltpu.PrefetchScalarGridSpec(
            num_scalar_prefetch=1,
            grid=(steps,),
            in_specs=[
                pl.BlockSpec((total_rows, hidden_width), lambda g, s: (0, 0)),
                pl.BlockSpec((None, hidden_width, width), lambda g, s: (0, 0, s[g])),
            ],
            out_specs=(
                pl.BlockSpec(
                    (None, total_rows, width), lambda g, s: (jnp.minimum(g, sends - 1), 0, 0)
                ),
                pl.BlockSpec(
                    (None, total_rows, width), lambda g, s: (jnp.maximum(g - sends, 0), 0, 0)
                ),
            ),
        ),
        compiler_params=pltpu.CompilerParams(
            dimension_semantics=("arbitrary",), vmem_limit_bytes=40 << 20
        ),
        name="down",
    )(blocks, hidden, down_weight)


def shards(
    head_outputs,
    stream,
    adapter_down_factors,
    adapter_up_factors,
    norm_gain_vector,
    router_matrix,
    token_adapter_index,
    token_expert_index,
    gate_weight,
    up_weight,
    down_weight,
):
    tok_rows, model_width = head_outputs.shape
    held_count = adapter_down_factors.shape[1] // ADAPTER_RANK
    experts = router_matrix.shape[1]
    groups = lax.axis_size("aa")
    peers = lax.axis_size("ba")
    index_aa = lax.axis_index("aa")
    index_ba = lax.axis_index("ba")
    width = model_width // groups
    halves = peers // experts
    f32, bf16 = jnp.float32, jnp.bfloat16

    def columns(array, owner):
        return lax.dynamic_slice_in_dim(array, owner * width, width, array.ndim - 1)

    up_parts = [columns(adapter_up_factors, index_aa)]
    for r in range(1, groups):
        up_parts.append(swap(columns(adapter_up_factors, index_aa ^ r), "aa", r))

    local_ids = token_adapter_index - index_aa * held_count
    column_holder = jnp.arange(adapter_down_factors.shape[1], dtype=jnp.int32) // ADAPTER_RANK
    low_rank = jnp.dot(head_outputs, adapter_down_factors, preferred_element_type=f32)
    low_rank = jnp.where(local_ids[:, None] == column_holder[None, :], low_rank, 0.0).astype(bf16)
    low_parts = [low_rank] + [swap(low_rank, "aa", r) for r in range(1, groups)]
    update = sum(
        jnp.dot(low, up, preferred_element_type=f32) for low, up in zip(low_parts, up_parts)
    )
    residual_share = columns(stream, index_aa).astype(f32) + ADAPTER_SCALE * update

    tallies = jnp.sum(
        (local_ids[:, None] == jnp.arange(held_count, dtype=jnp.int32)[None, :]).astype(f32),
        axis=0,
    )
    distance = 1
    while distance < peers:
        tallies = tallies + swap(tallies, "ba", distance)
        distance *= 2

    gain_share = columns(norm_gain_vector, index_aa)
    scaled = residual_share * gain_share
    router_share = lax.dynamic_slice_in_dim(router_matrix, index_aa * width, width, 0)
    logits = lax.dot_general(
        router_share, scaled.astype(bf16), (((0,), (1,)), ((), ())), preferred_element_type=f32
    )
    squares = jnp.sum(residual_share * residual_share, axis=1)[None, :]
    stats = jnp.concatenate([logits, squares], axis=0)
    stats = sum([stats] + [swap(stats, "aa", r) for r in range(1, groups)])
    inv_norm = lax.rsqrt(stats[experts] / model_width + EPS)
    normed = (scaled * inv_norm[:, None]).astype(bf16)
    logits = stats[:experts] * inv_norm[None, :]

    experts_iota = jnp.arange(experts, dtype=jnp.int32)
    chosen = (token_expert_index[:, :, None] == experts_iota[None, None, :]).astype(f32)
    picked = jnp.sum(chosen * logits.T[:, None, :], axis=2)
    weights = 1.0 / (1.0 + jnp.exp(picked[:, ::-1] - picked))
    flat_experts = token_expert_index.reshape(-1)
    expert_hits = (flat_experts[:, None] == experts_iota[None, :]).astype(jnp.int32)
    before = jnp.cumsum(expert_hits, axis=0) - expert_hits
    position = jnp.sum(before * expert_hits, axis=1)
    expert_of = (index_ba ^ jnp.arange(peers, dtype=jnp.int32)) // halves
    caps_iota = jnp.arange(CAP, dtype=jnp.int32)
    placed = (expert_of[:, None, None] == flat_experts[None, None, :]) & (
        position[None, None, :] == caps_iota[None, :, None]
    )
    placed = placed.reshape(peers, CAP, tok_rows, 2)
    pick_rows = jnp.any(placed, axis=3).astype(bf16)
    mixing = jnp.sum(jnp.where(placed, weights[None, None], 0.0), axis=3)

    near = peers // 2
    order = list(range(near, peers)) + list(range(near))
    received = [None] * peers
    for s in order:
        block = jnp.dot(pick_rows[s], normed, preferred_element_type=f32).astype(bf16)
        received[s] = swap(block, "ba", s) if s else block
    split = near + near // 2
    pieces, rows_of = [], []
    for first, last in ((0, near), (near, split), (split, peers)):
        own = jnp.concatenate(received[first:last], axis=0)
        held = [own] + [swap(own, "aa", r) for r in range(2, groups, 2)]
        for number, piece in enumerate(held):
            pieces += [piece, swap(piece, "aa", 1)]
            rows_of += [(first * CAP, 2 * number), (first * CAP, 2 * number + 1)]

    total_rows = peers * CAP
    offsets = index_aa ^ jnp.arange(groups, dtype=jnp.int32)
    hidden = gate_up(pieces, tuple(rows_of), offsets, gate_weight, up_weight, total_rows)

    part_width = width // COLUMN_CHUNKS
    pair_count = groups // 2
    quarters = jnp.concatenate([offsets[1::2], offsets[0::2]])
    outcome = []
    for chunk in range(COLUMN_CHUNKS):
        send, keep = down(
            hidden, quarters * COLUMN_CHUNKS + chunk, down_weight, part_width, pair_count
        )
        keep = keep + swap(send, "aa", 1).astype(f32)
        total = keep[0]
        for number in range(1, pair_count):
            total = total + swap(keep[number].astype(bf16), "aa", 2 * number).astype(f32)
        total = total.astype(bf16).reshape(peers, CAP, part_width)
        returned = jnp.concatenate(
            [swap(total[s], "ba", s) if s else total[s] for s in range(peers)], axis=0
        )
        flat = mixing.reshape(peers * CAP, tok_rows)
        gathered = jnp.zeros((tok_rows, part_width), f32)
        for _ in range(3):
            high = flat.astype(bf16)
            flat = flat - high.astype(f32)
            gathered = gathered + lax.dot_general(
                high, returned, (((0,), (0,)), ((), ())), preferred_element_type=f32
            )
        outcome.append(gathered)
    mixed_share = residual_share + jnp.concatenate(outcome, axis=1)
    return (mixed_share.astype(bf16), tallies)


def solution(mesh):
    in_specs = (
        P("ba", None),
        P("ba", None),
        P(None, "aa"),
        P("aa", None),
        P(),
        P(),
        P("ba"),
        P("ba", None),
        P("ba", None, "aa"),
        P("ba", None, "aa"),
        P("ba", "aa", None),
    )
    out_specs = (P("ba", "aa"), P("aa"))
    return jax.shard_map(shards, mesh=mesh, in_specs=in_specs, out_specs=out_specs, check_vma=False)
```

```python
import functools

import jax
import jax.numpy as jnp
from jax import lax
from jax.experimental import pallas as pl
from jax.experimental.pallas import tpu as pltpu
from jax.sharding import PartitionSpec as P


ADAPTER_RANK = 16
CAP = 48

EPS = 1e-05
ADAPTER_SCALE = 2.0
LANES = 128
RING = 6


def swap(value, axis, distance):
    size = lax.axis_size(axis)
    return lax.ppermute(value, axis, [(k, k ^ distance) for k in range(size)])


def tile_of(width, most):
    tile = most
    while width % tile:
        tile //= 2
    return tile


def expert_kernel(offset_ref, gain_hbm, *refs, groups, rows_of, owners):
    count = len(rows_of)
    number_of_groups = len(groups)
    pieces, refs = refs[:count], refs[count:]
    gate_ref, up_ref, down_ref = refs[:3]
    send_refs = refs[3 : 3 + number_of_groups]
    keep_refs = refs[3 + number_of_groups : 3 + 2 * number_of_groups]
    x_ref, hidden_ref, inv_ref, gain_ref, ring_ref, piece_sem, ring_sem = refs[
        3 + 2 * number_of_groups :
    ]
    total_rows, model_width = x_ref.shape
    hidden_width = hidden_ref.shape[1]
    slots, _, tile = ring_ref.shape
    width = model_width // owners
    share = width // tile
    pairs = hidden_width // tile
    down_tiles = model_width // tile
    sends = down_tiles // 2
    ahead = slots // 2

    def gate_copy(n):
        slot = (2 * n) % slots
        return pltpu.make_async_copy(
            gate_ref.at[0, :, pl.ds(n * tile, tile)], ring_ref.at[slot], ring_sem.at[slot]
        )

    def up_copy(n):
        slot = (2 * n + 1) % slots
        return pltpu.make_async_copy(
            up_ref.at[0, :, pl.ds(n * tile, tile)], ring_ref.at[slot], ring_sem.at[slot]
        )

    def down_copy(d):
        slot = (2 * pairs + d) % slots
        order = d // share
        index = jnp.where(d < sends, 2 * order + 1, 2 * (order - owners // 2))
        column = offset_ref[index] * share + d % share
        return pltpu.make_async_copy(
            down_ref.at[0, :, pl.ds(column * tile, tile)],
            ring_ref.at[slot, pl.ds(0, hidden_width), :],
            ring_sem.at[slot],
        )

    copies = [pltpu.make_async_copy(gain_hbm, gain_ref, piece_sem.at[count])]
    for number, piece in enumerate(pieces):
        first, index = rows_of[number]
        start = pl.multiple_of(offset_ref[index] * width, LANES)
        copies.append(
            pltpu.make_async_copy(
                piece,
                x_ref.at[pl.ds(first, piece.shape[0]), pl.ds(start, width)],
                piece_sem.at[number],
            )
        )
    for copy in copies:
        copy.start()
    for n in range(ahead):
        if n < pairs:
            gate_copy(n).start()
            up_copy(n).start()
        else:
            down_copy(2 * (n - pairs)).start()
            down_copy(2 * (n - pairs) + 1).start()
    for copy in copies:
        copy.wait()

    chunk = 16
    gain_ref[...] = 1.0 / gain_ref[...]

    def norm_step(c, carry):
        rows = pl.ds(pl.multiple_of(c * chunk, chunk), chunk)
        values = x_ref[rows, :].astype(jnp.float32) * gain_ref[...]
        mean = jnp.sum(values * values, axis=1, keepdims=True) / model_width
        inv_ref[rows, :] = jnp.broadcast_to(lax.rsqrt(mean + EPS), (chunk, LANES))
        return carry

    lax.fori_loop(0, total_rows // chunk, norm_step, 0)

    def pair_step(n, carry):
        rows = x_ref[...]
        inv = inv_ref[:, :1]
        gate_copy(n).wait()
        up_copy(n).wait()
        gate = jnp.dot(rows, ring_ref[(2 * n) % slots], preferred_element_type=jnp.float32)
        up = jnp.dot(rows, ring_ref[(2 * n + 1) % slots], preferred_element_type=jnp.float32)
        gate = gate * inv
        value = (gate / (1.0 + jnp.exp(-gate))) * (up * inv)
        hidden_ref[:, pl.ds(pl.multiple_of(n * tile, tile), tile)] = value.astype(jnp.bfloat16)
        later = n + ahead

        @pl.when(later < pairs)
        def _():
            gate_copy(later).start()
            up_copy(later).start()

        @pl.when((later >= pairs) & (2 * (later - pairs) < down_tiles))
        def _():
            down_copy(2 * (later - pairs)).start()
            down_copy(2 * (later - pairs) + 1).start()

        return carry

    lax.fori_loop(0, pairs, pair_step, 0)

    def phase(base, out_refs):
        def down_step(d, carry):
            slot = (2 * pairs + base + d) % slots
            down_copy(base + d).wait()
            part = jnp.dot(
                hidden_ref[...],
                ring_ref[slot, pl.ds(0, hidden_width), :],
                preferred_element_type=jnp.float32,
            )
            start = pl.multiple_of((d % share) * tile, tile)
            for out_ref, (first, rows) in zip(out_refs, groups):
                out_ref[d // share, :, pl.ds(start, tile)] = part[first : first + rows].astype(
                    out_ref.dtype
                )
            later = base + d + 2 * ahead

            @pl.when(later < down_tiles)
            def _():
                down_copy(later).start()

            return carry

        lax.fori_loop(0, sends, down_step, 0)

    phase(0, send_refs)
    phase(sends, keep_refs)


def expert_rows(pieces, rows_of, groups, offsets, gain, gate_weight, up_weight, down_weight):
    model_width, hidden_width = gate_weight.shape[1:]
    owners = offsets.shape[0]
    width = model_width // owners
    total_rows = sum(rows for _, rows in groups)
    tile = tile_of(hidden_width, 512)
    while width % tile or ((model_width // tile) // 2) % 2:
        tile //= 2
    bf16, f32 = jnp.bfloat16, jnp.float32
    return pl.pallas_call(
        functools.partial(expert_kernel, groups=groups, rows_of=rows_of, owners=owners),
        out_shape=[jax.ShapeDtypeStruct((owners // 2, rows, width), bf16) for _, rows in groups]
        + [jax.ShapeDtypeStruct((owners // 2, rows, width), f32) for _, rows in groups],
        in_specs=[pl.BlockSpec(memory_space=pltpu.SMEM), pl.BlockSpec(memory_space=pltpu.HBM)]
        + [pl.BlockSpec(memory_space=pl.ANY)] * len(pieces)
        + [pl.BlockSpec(memory_space=pltpu.HBM)] * 3,
        out_specs=[pl.BlockSpec(memory_space=pltpu.VMEM)] * (2 * len(groups)),
        scratch_shapes=[
            pltpu.VMEM((total_rows, model_width), bf16),
            pltpu.VMEM((total_rows, hidden_width), bf16),
            pltpu.VMEM((total_rows, LANES), f32),
            pltpu.VMEM((1, model_width), f32),
            pltpu.VMEM((RING, model_width, tile), bf16),
            pltpu.SemaphoreType.DMA((len(pieces) + 1,)),
            pltpu.SemaphoreType.DMA((RING,)),
        ],
        compiler_params=pltpu.CompilerParams(vmem_limit_bytes=45 << 20),
        name="expert_rows",
    )(offsets, gain, *pieces, gate_weight, up_weight, down_weight)


def with_adapter(rows, up_refs, spread_ref, adapter_ref, width):
    held = up_refs[0].shape[0]
    low = rows[:, width : width + ADAPTER_RANK]
    ids = rows[:, width + ADAPTER_RANK : width + ADAPTER_RANK + 1].astype(jnp.float32)
    wide = jnp.dot(low, spread_ref[...], preferred_element_type=jnp.float32)
    wide = jnp.where(ids == adapter_ref[...].astype(jnp.float32), wide, 0.0).astype(jnp.bfloat16)
    update = sum(
        jnp.dot(wide[:, k * held : (k + 1) * held], up[...], preferred_element_type=jnp.float32)
        for k, up in enumerate(up_refs)
    )
    return rows[:, :width].astype(jnp.float32) + ADAPTER_SCALE * update


def adapter_kernel(*refs, blocks):
    block_refs, up_refs = refs[:blocks], refs[blocks:-4]
    spread_ref, adapter_ref, gain_ref, out_ref = refs[-4:]
    width = out_ref.shape[1]
    rows = jnp.concatenate([block[...] for block in block_refs], axis=0)
    total = with_adapter(rows, up_refs, spread_ref, adapter_ref, width)
    out_ref[...] = (total * gain_ref[...]).astype(jnp.bfloat16)


def adapter_rows(blocks, up_parts, spread, adapter_of, gain):
    rows = sum(block.shape[0] for block in blocks)
    return pl.pallas_call(
        functools.partial(adapter_kernel, blocks=len(blocks)),
        out_shape=jax.ShapeDtypeStruct((rows, gain.shape[1]), jnp.bfloat16),
        compiler_params=pltpu.CompilerParams(vmem_limit_bytes=16 << 20),
        name="adapter_rows",
    )(*blocks, *up_parts, spread, adapter_of, gain)


def total_kernel(keep_ref, other_ref, *refs, count):
    part_refs, out_refs = refs[:count], refs[count:]
    rows = out_refs[0].shape[0]
    for k, out_ref in enumerate(out_refs):
        span = pl.ds(k * rows, rows)
        total = keep_ref[0, span, :] + other_ref[0, span, :].astype(jnp.float32)
        for part_ref in part_refs:
            total = total + part_ref[span, :].astype(jnp.float32)
        out_ref[...] = total.astype(jnp.bfloat16)


def total_rows_of(keep, other, parts, blocks):
    _, rows, width = keep.shape
    first = pl.BlockSpec((1, rows, width), lambda n: (0, 0, 0))
    whole = pl.BlockSpec((rows, width), lambda n: (0, 0))
    block = pl.BlockSpec((rows // blocks, width), lambda n: (0, 0))
    return pl.pallas_call(
        functools.partial(total_kernel, count=len(parts)),
        grid=(1,),
        out_shape=[jax.ShapeDtypeStruct((rows // blocks, width), jnp.bfloat16)] * blocks,
        in_specs=[first, first] + [whole] * len(parts),
        out_specs=[block] * blocks,
        compiler_params=pltpu.CompilerParams(vmem_limit_bytes=16 << 20),
        name="total_rows",
    )(keep, other, *parts)


def column_copy(source, first, width, target, sem):
    start = pl.multiple_of(first * width, LANES)
    return pltpu.make_async_copy(source.at[:, pl.ds(start, width)], target, sem)


def ids_by_row(ids_row):
    tokens = ids_row.shape[1]
    return jnp.broadcast_to(ids_row.astype(jnp.float32), (LANES, tokens)).T


def front_kernel(
    place_ref, ids_ref, experts_ref, head_hbm, down_hbm, up_ref, stream_ref, *refs, owners, sizes
):
    low_ref, stream_out, pick_ref, extra_ref, target_ref = refs[:5]
    up_outs = refs[5:-3]
    head_ref, down_ref, sem = refs[-3:]
    width = stream_out.shape[1]
    held_width = down_ref.shape[1]
    owner = place_ref[0]
    first_copies = [
        pltpu.make_async_copy(head_hbm, head_ref, sem.at[owners + 1]),
        pltpu.make_async_copy(down_hbm, down_ref, sem.at[owners + 2]),
    ]
    copies = [column_copy(stream_ref, owner, width, stream_out, sem.at[owners])]
    for r, out in enumerate(up_outs):
        copies.append(column_copy(up_ref, owner ^ r, width, out, sem.at[r]))
    for copy in first_copies + copies:
        copy.start()
    f32, i32 = jnp.float32, jnp.int32
    experts, halves = sizes
    tokens = ids_ref.shape[1]
    ids = ids_by_row(ids_ref[...])
    lanes = lax.broadcasted_iota(i32, (tokens, LANES), 1)
    held = held_width // ADAPTER_RANK
    lane_held = lanes - 2 * ADAPTER_RANK
    wanted = jnp.where((lane_held >= 0) & (lane_held < held), owner * held + lane_held, -1)
    tally = jnp.sum(jnp.where(ids == wanted.astype(f32), 1.0, 0.0), axis=0, keepdims=True)
    extra_ref[0:tokens, :] = jnp.where(lanes == ADAPTER_RANK, ids, 0.0)
    extra_ref[tokens : tokens + 8, :] = jnp.broadcast_to(tally, (8, LANES))

    names = lax.broadcasted_iota(i32, (experts, tokens), 0)
    hits = [experts_ref[k : k + 1, :] == names for k in range(2)]
    both = jnp.where(hits[0] | hits[1], 1.0, 0.0)
    square = (tokens, tokens)
    earlier = lax.broadcasted_iota(i32, square, 0) < lax.broadcasted_iota(i32, square, 1)
    before = jnp.dot(
        both.astype(jnp.bfloat16),
        jnp.where(earlier, 1.0, 0.0).astype(jnp.bfloat16),
        preferred_element_type=f32,
    )
    targets, chosen = [], []
    for k in range(2):
        position = jnp.sum(jnp.where(hits[k], before, 0.0), axis=0, keepdims=True).astype(i32)
        chosen.append(experts_ref[k : k + 1, :].astype(f32))
        for half in range(halves):
            slot = (experts_ref[k : k + 1, :] * halves + half) ^ place_ref[1]
            targets.append(slot * CAP + position)
    rows = lax.broadcasted_iota(i32, pick_ref.shape, 0)
    pick = functools.reduce(jnp.logical_or, [rows == target for target in targets])
    pick_ref[...] = jnp.where(pick, 1.0, 0.0).astype(jnp.bfloat16)
    filled = jnp.zeros((LANES - len(targets) - 2, tokens), f32)
    target_ref[...] = jnp.concatenate(
        chosen + [target.astype(f32) for target in targets] + [filled], axis=0
    ).T
    for copy in first_copies:
        copy.wait()
    low = jnp.dot(head_ref[...], down_ref[...], preferred_element_type=jnp.float32)
    lane = lax.broadcasted_iota(jnp.int32, (low.shape[0], LANES), 1)
    first = owner * held
    masked = []
    for start in range(0, held_width, LANES):
        adapter = (first + (lane + start) // ADAPTER_RANK).astype(jnp.float32)
        masked.append(jnp.where(ids == adapter, low[:, start : start + LANES], 0.0))
    low = jnp.concatenate(masked, axis=1).astype(jnp.bfloat16)
    fold_shape = (ADAPTER_RANK, held_width)
    fold = lax.broadcasted_iota(jnp.int32, fold_shape, 1) % ADAPTER_RANK
    fold = jnp.where(fold == lax.broadcasted_iota(jnp.int32, fold_shape, 0), 1.0, 0.0)
    low_ref[...] = lax.dot_general(
        fold.astype(jnp.bfloat16),
        low,
        (((1,), (1,)), ((), ())),
        preferred_element_type=jnp.float32,
    ).astype(jnp.bfloat16)
    for copy in copies:
        copy.wait()


def front(place, head_outputs, down_factors, ids, experts_of, up_factors, stream, owners, sizes):
    rows, model_width = head_outputs.shape
    total_rows = sizes[0] * sizes[1] * CAP
    width = model_width // owners
    bf16 = jnp.bfloat16
    vmem, hbm = pl.BlockSpec(memory_space=pltpu.VMEM), pl.BlockSpec(memory_space=pltpu.HBM)
    return pl.pallas_call(
        functools.partial(front_kernel, owners=owners, sizes=sizes),
        out_shape=[
            jax.ShapeDtypeStruct((ADAPTER_RANK, rows), bf16),
            jax.ShapeDtypeStruct((rows, width), bf16),
            jax.ShapeDtypeStruct((total_rows, rows), bf16),
            jax.ShapeDtypeStruct((rows + 8, LANES), jnp.float32),
            jax.ShapeDtypeStruct((rows, LANES), jnp.float32),
        ]
        + [jax.ShapeDtypeStruct((up_factors.shape[0], width), bf16)] * owners,
        in_specs=[pl.BlockSpec(memory_space=pltpu.SMEM), vmem, vmem] + [hbm] * 4,
        out_specs=[vmem] * (5 + owners),
        scratch_shapes=[
            pltpu.VMEM(head_outputs.shape, bf16),
            pltpu.VMEM(down_factors.shape, bf16),
            pltpu.SemaphoreType.DMA((owners + 3,)),
        ],
        compiler_params=pltpu.CompilerParams(vmem_limit_bytes=52 << 20),
        name="front",
    )(place, ids[None, :], experts_of.T, head_outputs, down_factors, up_factors, stream)


def route_kernel(pick_ref, extra_ref, stream_ref, *refs, owners):
    low_refs, payload_ref, out_refs = refs[:owners], refs[owners], refs[owners + 1 :]
    f32, bf16 = jnp.float32, jnp.bfloat16
    tokens, width = stream_ref.shape
    low = sum(ref[...].astype(f32) for ref in low_refs)
    lows = jnp.concatenate([low, jnp.zeros((LANES - ADAPTER_RANK, tokens), f32)], axis=0).T
    extra = extra_ref[...]
    tail = (lows + extra[:tokens]).astype(bf16)
    tally = extra[tokens : tokens + 1]
    pick = pick_ref[...]
    payload_ref[:, pl.ds(0, width)] = stream_ref[...]
    payload_ref[:, pl.ds(width, LANES)] = tail

    moved = jnp.dot(pick, stream_ref[...], preferred_element_type=f32).astype(bf16)
    moved_tail = (jnp.dot(pick, tail, preferred_element_type=f32) + tally).astype(bf16)
    for s, out_ref in enumerate(out_refs):
        out_ref[:, pl.ds(0, width)] = moved[s * CAP : (s + 1) * CAP]
        out_ref[:, pl.ds(width, LANES)] = moved_tail[s * CAP : (s + 1) * CAP]


def route(pick, extra, stream_share, low_parts, peers):
    tokens, width = stream_share.shape
    bf16 = jnp.bfloat16
    vmem = pl.BlockSpec(memory_space=pltpu.VMEM)
    return pl.pallas_call(
        functools.partial(route_kernel, owners=len(low_parts)),
        out_shape=[jax.ShapeDtypeStruct((tokens, width + LANES), bf16)]
        + [jax.ShapeDtypeStruct((CAP, width + LANES), bf16)] * peers,
        in_specs=[vmem] * (3 + len(low_parts)),
        out_specs=[vmem] * (1 + peers),
        compiler_params=pltpu.CompilerParams(vmem_limit_bytes=16 << 20),
        name="route",
    )(pick, extra, stream_share, *low_parts)


def own_kernel(payload_ref, *refs):
    up_refs = refs[:-6]
    spread_ref, adapter_ref, gain_ref, router_ref, residual_ref, stats_ref = refs[-6:]
    rows = payload_ref[...]
    total = with_adapter(rows, up_refs, spread_ref, adapter_ref, gain_ref.shape[1])
    residual_ref[...] = total
    scaled = (total * gain_ref[...]).astype(jnp.bfloat16)
    squares = jnp.sum(total * total, axis=1, keepdims=True)
    logits = lax.dot_general(
        router_ref[...], scaled, (((1,), (1,)), ((), ())), preferred_element_type=jnp.float32
    )
    experts = logits.shape[0]
    stats_ref[0:experts, :] = logits
    squares = jnp.broadcast_to(squares, (squares.shape[0], LANES)).T
    stats_ref[experts : 2 * experts, :] = squares[:experts]


def own_rows(payload, up_parts, spread, adapter_of, gain, router):
    tokens, width = payload.shape[0], gain.shape[1]
    return pl.pallas_call(
        own_kernel,
        out_shape=[
            jax.ShapeDtypeStruct((tokens, width), jnp.float32),
            jax.ShapeDtypeStruct((2 * router.shape[0], tokens), jnp.float32),
        ],
        compiler_params=pltpu.CompilerParams(vmem_limit_bytes=16 << 20),
        name="own_rows",
    )(payload, *up_parts, spread, adapter_of, gain, router)


def mix_kernel(target_ref, *refs, blocks, halves, model_width):
    stat_refs, block_refs = refs[: -3 - blocks], refs[-3 - blocks : -3]
    high_ref, rest_ref, load_ref = refs[-3:]
    f32 = jnp.float32
    stats = sum(ref[...] for ref in stat_refs)
    count, tokens = stats.shape
    stats = jnp.concatenate([stats, jnp.zeros((LANES - count, tokens), f32)], axis=0).T
    inv = lax.rsqrt(stats[:, count // 2 : count // 2 + 1] / model_width + EPS)
    lane = lax.broadcasted_iota(jnp.int32, stats.shape, 1).astype(f32)
    picked = [
        jnp.sum(
            jnp.where(target_ref[:, k : k + 1] == lane, stats * inv, 0.0), axis=1, keepdims=True
        )
        for k in range(2)
    ]
    slots = lax.broadcasted_iota(jnp.int32, high_ref.shape, 1).astype(f32)
    mixing = jnp.zeros(high_ref.shape, f32)
    for k in range(2):
        weight = 1.0 / (1.0 + jnp.exp(picked[1 - k] - picked[k]))
        for half in range(halves):
            column = 2 + k * halves + half
            mixing = jnp.where(slots == target_ref[:, column : column + 1], weight, mixing)
    high = mixing.astype(jnp.bfloat16)
    high_ref[...] = high
    rest_ref[...] = (mixing - high.astype(f32)).astype(jnp.bfloat16)
    load_ref[...] = sum(ref[...].astype(f32)[:1, :] for ref in block_refs)


def mix(targets, stats, blocks, experts, model_width):
    tokens = targets.shape[0]
    peers = len(blocks)
    width = blocks[0].shape[1] - LANES
    total_rows = peers * CAP
    full = lambda shape: pl.BlockSpec(shape, lambda n: (0,) * len(shape))
    corner = pl.BlockSpec((16, LANES), lambda n: (0, width // LANES))
    return pl.pallas_call(
        functools.partial(
            mix_kernel, blocks=peers, halves=peers // experts, model_width=model_width
        ),
        grid=(1,),
        out_shape=[jax.ShapeDtypeStruct((tokens, total_rows), jnp.bfloat16)] * 2
        + [jax.ShapeDtypeStruct((1, LANES), jnp.float32)],
        in_specs=[full(targets.shape)]
        + [full(stat.shape) for stat in stats]
        + [corner] * peers,
        out_specs=[full((tokens, total_rows))] * 2 + [full((1, LANES))],
        compiler_params=pltpu.CompilerParams(vmem_limit_bytes=16 << 20),
        name="mix",
    )(targets, *stats, *blocks)


def finish_kernel(residual_ref, high_ref, rest_ref, *refs):
    block_refs, out_ref = refs[:-1], refs[-1]
    rows = jnp.concatenate([ref[...] for ref in block_refs], axis=0)
    total = jnp.dot(rest_ref[...], rows, preferred_element_type=jnp.float32)
    total = total + jnp.dot(high_ref[...], rows, preferred_element_type=jnp.float32)
    out_ref[...] = (residual_ref[...] + total).astype(out_ref.dtype)


def finish(residual, high, rest, blocks):
    return pl.pallas_call(
        finish_kernel,
        out_shape=jax.ShapeDtypeStruct(residual.shape, jnp.bfloat16),
        compiler_params=pltpu.CompilerParams(vmem_limit_bytes=16 << 20),
        name="finish",
    )(residual, high, rest, *blocks)


def shards(
    head_outputs,
    stream,
    adapter_down_factors,
    adapter_up_factors,
    norm_gain_vector,
    router_matrix,
    token_adapter_index,
    token_expert_index,
    gate_weight,
    up_weight,
    down_weight,
):
    _, model_width = head_outputs.shape
    held_width = adapter_down_factors.shape[1]
    held_count = held_width // ADAPTER_RANK
    experts = router_matrix.shape[1]
    owners = lax.axis_size("aa")
    peers = lax.axis_size("ba")
    index_aa = lax.axis_index("aa")
    index_ba = lax.axis_index("ba")
    width = model_width // owners
    f32, bf16, i32 = jnp.float32, jnp.bfloat16, jnp.int32

    place = jnp.stack([index_aa, index_ba])
    low, stream_share, pick, extra, targets, *up_parts = front(
        place,
        head_outputs,
        adapter_down_factors,
        token_adapter_index,
        token_expert_index,
        adapter_up_factors,
        stream,
        owners,
        (experts, peers // experts),
    )
    low_parts = [low] + [swap(low, "aa", r) for r in range(1, owners)]
    up_parts = [up_parts[0]] + [swap(up_parts[r], "aa", r) for r in range(1, owners)]
    spots = jnp.arange(owners * held_width, dtype=i32)
    adapter_of = (index_aa ^ (spots // held_width)) * held_count + (
        spots % held_width
    ) // ADAPTER_RANK
    adapter_of = adapter_of[None, :]
    spread = (jnp.arange(ADAPTER_RANK, dtype=i32)[:, None] == spots[None, :] % ADAPTER_RANK).astype(
        bf16
    )

    payload, *outgoing = route(pick, extra, stream_share, low_parts, peers)
    near = peers // 2
    split = near + near // 2
    received = [swap(block, "ba", s) if s else block for s, block in enumerate(outgoing)]

    gain = lax.dynamic_slice_in_dim(norm_gain_vector, index_aa * width, width, 0)[None, :]
    pieces, rows_of, groups = [], [], []
    spans = ((0, near), (near, split), (split, peers))
    for first, last in spans:
        own = adapter_rows(received[first:last], up_parts, spread, adapter_of, gain)
        held = [own] + [swap(own, "aa", r) for r in range(2, owners, 2)]
        groups.append((first * CAP, (last - first) * CAP))
        for number, piece in enumerate(held):
            pieces += [piece, swap(piece, "aa", 1)]
            rows_of += [(first * CAP, 2 * number), (first * CAP, 2 * number + 1)]

    router = lax.dynamic_slice_in_dim(router_matrix.T, index_aa * width, width, 1)
    residual_share, stats = own_rows(payload, up_parts, spread, adapter_of, gain, router)
    stats = [stats] + [swap(stats, "aa", r) for r in range(1, owners)]
    high, rest, load = mix(targets, stats, received, experts, model_width)
    adapter_load = load[0, 2 * ADAPTER_RANK : 2 * ADAPTER_RANK + held_count]

    offsets = index_aa ^ jnp.arange(owners, dtype=i32)
    results = expert_rows(
        pieces,
        tuple(rows_of),
        tuple(groups),
        offsets,
        norm_gain_vector[None, :],
        gate_weight,
        up_weight,
        down_weight,
    )

    returned = [None] * peers
    for g in (1, 2, 0):
        first, last = spans[g]
        send, keep = results[g], results[len(groups) + g]
        other = swap(send, "aa", 1)
        parts = [
            swap((keep[d] + other[d].astype(f32)).astype(bf16), "aa", 2 * d)
            for d in range(1, owners // 2)
        ]
        blocks = total_rows_of(keep, other, parts, last - first)
        for s, block in zip(range(first, last), blocks):
            returned[s] = swap(block, "ba", s) if s else block
    return (finish(residual_share, high, rest, returned), adapter_load)


def solution(mesh):
    in_specs = (
        P("ba", None),
        P("ba", None),
        P(None, "aa"),
        P("aa", None),
        P(),
        P(),
        P("ba"),
        P("ba", None),
        P("ba", None, "aa"),
        P("ba", None, "aa"),
        P("ba", "aa", None),
    )
    out_specs = (P("ba", "aa"), P("aa"))

    return jax.shard_map(shards, mesh=mesh, in_specs=in_specs, out_specs=out_specs, check_vma=False)
```

```python
import functools

import jax
import jax.numpy as jnp
from jax import lax
from jax.experimental import pallas as pl
from jax.experimental.pallas import tpu as pltpu
from jax.sharding import PartitionSpec as P


ADAPTER_RANK = 16
CAP = 48

EPS = 1e-05
ADAPTER_SCALE = 2.0
LANES = 128
RING = 6


def swap(value, axis, distance):
    size = lax.axis_size(axis)
    return lax.ppermute(value, axis, [(k, k ^ distance) for k in range(size)])


def tile_of(width, most):
    tile = most
    while width % tile:
        tile //= 2
    return tile


def expert_kernel(offset_ref, inverse_ref, *refs, groups, rows_of, owners):
    count = len(rows_of)
    number_of_groups = len(groups)
    pieces, refs = refs[:count], refs[count:]
    gate_ref, up_ref, down_ref = refs[:3]
    send_refs = refs[3 : 3 + number_of_groups]
    keep_refs = refs[3 + number_of_groups : 3 + 2 * number_of_groups]
    x_ref, hidden_ref, inv_ref, ring_ref, piece_sem, ring_sem = refs[
        3 + 2 * number_of_groups :
    ]
    total_rows, model_width = x_ref.shape
    hidden_width = hidden_ref.shape[1]
    slots, _, tile = ring_ref.shape
    width = model_width // owners
    share = width // tile
    pairs = hidden_width // tile
    down_tiles = model_width // tile
    sends = down_tiles // 2
    ahead = slots // 2

    def gate_copy(n):
        slot = (2 * n) % slots
        return pltpu.make_async_copy(
            gate_ref.at[0, :, pl.ds(n * tile, tile)], ring_ref.at[slot], ring_sem.at[slot]
        )

    def up_copy(n):
        slot = (2 * n + 1) % slots
        return pltpu.make_async_copy(
            up_ref.at[0, :, pl.ds(n * tile, tile)], ring_ref.at[slot], ring_sem.at[slot]
        )

    def down_copy(d):
        slot = (2 * pairs + d) % slots
        order = d // share
        index = jnp.where(d < sends, 2 * order + 1, 2 * (order - owners // 2))
        column = offset_ref[index] * share + d % share
        return pltpu.make_async_copy(
            down_ref.at[0, :, pl.ds(column * tile, tile)],
            ring_ref.at[slot, pl.ds(0, hidden_width), :],
            ring_sem.at[slot],
        )

    copies = []
    for number, piece in enumerate(pieces):
        first, index = rows_of[number]
        start = pl.multiple_of(offset_ref[index] * width, LANES)
        copies.append(
            pltpu.make_async_copy(
                piece,
                x_ref.at[pl.ds(first, piece.shape[0]), pl.ds(start, width)],
                piece_sem.at[number],
            )
        )

    def fetch(n):
        if n < pairs:
            gate_copy(n).start()
            up_copy(n).start()
        else:
            down_copy(2 * (n - pairs)).start()
            down_copy(2 * (n - pairs) + 1).start()

    fetch(0)
    for copy in copies:
        copy.start()
    for n in range(1, ahead):
        fetch(n)
    for copy in copies:
        copy.wait()

    chunk = 16

    def norm_step(c, carry):
        rows = pl.ds(pl.multiple_of(c * chunk, chunk), chunk)
        values = x_ref[rows, :].astype(jnp.float32) * inverse_ref[...]
        mean = jnp.sum(values * values, axis=1, keepdims=True) / model_width
        inv_ref[rows, :] = jnp.broadcast_to(lax.rsqrt(mean + EPS), (chunk, LANES))
        return carry

    lax.fori_loop(0, total_rows // chunk, norm_step, 0)

    def pair_step(n, carry):
        rows = x_ref[...]
        inv = inv_ref[:, :1]
        gate_copy(n).wait()
        up_copy(n).wait()
        gate = jnp.dot(rows, ring_ref[(2 * n) % slots], preferred_element_type=jnp.float32)
        up = jnp.dot(rows, ring_ref[(2 * n + 1) % slots], preferred_element_type=jnp.float32)
        gate = gate * inv
        value = (gate / (1.0 + jnp.exp(-gate))) * (up * inv)
        hidden_ref[:, pl.ds(pl.multiple_of(n * tile, tile), tile)] = value.astype(jnp.bfloat16)
        later = n + ahead

        @pl.when(later < pairs)
        def _():
            gate_copy(later).start()
            up_copy(later).start()

        @pl.when((later >= pairs) & (2 * (later - pairs) < down_tiles))
        def _():
            down_copy(2 * (later - pairs)).start()
            down_copy(2 * (later - pairs) + 1).start()

        return carry

    lax.fori_loop(0, pairs, pair_step, 0)

    def phase(base, out_refs):
        def down_step(d, carry):
            slot = (2 * pairs + base + d) % slots
            down_copy(base + d).wait()
            part = jnp.dot(
                hidden_ref[...],
                ring_ref[slot, pl.ds(0, hidden_width), :],
                preferred_element_type=jnp.float32,
            )
            start = pl.multiple_of((d % share) * tile, tile)
            for out_ref, (first, rows) in zip(out_refs, groups):
                out_ref[d // share, :, pl.ds(start, tile)] = part[first : first + rows].astype(
                    out_ref.dtype
                )
            later = base + d + 2 * ahead

            @pl.when(later < down_tiles)
            def _():
                down_copy(later).start()

            return carry

        lax.fori_loop(0, sends, down_step, 0)

    phase(0, send_refs)
    phase(sends, keep_refs)


def expert_rows(pieces, rows_of, groups, offsets, inverse, gate_weight, up_weight, down_weight):
    model_width, hidden_width = gate_weight.shape[1:]
    owners = offsets.shape[0]
    width = model_width // owners
    total_rows = sum(rows for _, rows in groups)
    tile = tile_of(hidden_width, 512)
    while width % tile or ((model_width // tile) // 2) % 2:
        tile //= 2
    bf16, f32 = jnp.bfloat16, jnp.float32
    return pl.pallas_call(
        functools.partial(expert_kernel, groups=groups, rows_of=rows_of, owners=owners),
        out_shape=[jax.ShapeDtypeStruct((owners // 2, rows, width), bf16) for _, rows in groups]
        + [jax.ShapeDtypeStruct((owners // 2, rows, width), f32) for _, rows in groups],
        in_specs=[pl.BlockSpec(memory_space=pltpu.SMEM), pl.BlockSpec(memory_space=pltpu.VMEM)]
        + [pl.BlockSpec(memory_space=pl.ANY)] * len(pieces)
        + [pl.BlockSpec(memory_space=pltpu.HBM)] * 3,
        out_specs=[pl.BlockSpec(memory_space=pltpu.VMEM)] * (2 * len(groups)),
        scratch_shapes=[
            pltpu.VMEM((total_rows, model_width), bf16),
            pltpu.VMEM((total_rows, hidden_width), bf16),
            pltpu.VMEM((total_rows, LANES), f32),
            pltpu.VMEM((RING, model_width, tile), bf16),
            pltpu.SemaphoreType.DMA((len(pieces),)),
            pltpu.SemaphoreType.DMA((RING,)),
        ],
        compiler_params=pltpu.CompilerParams(vmem_limit_bytes=45 << 20),
        name="expert_rows",
    )(offsets, inverse, *pieces, gate_weight, up_weight, down_weight)


def with_adapter(rows, up_refs, spread_ref, adapter_ref, width):
    held = up_refs[0].shape[0]
    low = rows[:, width : width + ADAPTER_RANK]
    ids = rows[:, width + ADAPTER_RANK : width + ADAPTER_RANK + 1].astype(jnp.float32)
    wide = jnp.dot(low, spread_ref[...], preferred_element_type=jnp.float32)
    wide = jnp.where(ids == adapter_ref[...].astype(jnp.float32), wide, 0.0).astype(jnp.bfloat16)
    update = sum(
        jnp.dot(wide[:, k * held : (k + 1) * held], up[...], preferred_element_type=jnp.float32)
        for k, up in enumerate(up_refs)
    )
    return rows[:, :width].astype(jnp.float32) + ADAPTER_SCALE * update


def adapter_kernel(*refs, blocks):
    block_refs, up_refs = refs[:blocks], refs[blocks:-4]
    spread_ref, adapter_ref, gain_ref, out_ref = refs[-4:]
    width = out_ref.shape[1]
    rows = jnp.concatenate([block[...] for block in block_refs], axis=0)
    total = with_adapter(rows, up_refs, spread_ref, adapter_ref, width)
    out_ref[...] = (total * gain_ref[...]).astype(jnp.bfloat16)


def adapter_rows(blocks, up_parts, spread, adapter_of, gain):
    rows = sum(block.shape[0] for block in blocks)
    return pl.pallas_call(
        functools.partial(adapter_kernel, blocks=len(blocks)),
        out_shape=jax.ShapeDtypeStruct((rows, gain.shape[1]), jnp.bfloat16),
        compiler_params=pltpu.CompilerParams(vmem_limit_bytes=16 << 20),
        name="adapter_rows",
    )(*blocks, *up_parts, spread, adapter_of, gain)


def total_kernel(keep_ref, other_ref, *refs, count):
    part_refs, out_refs = refs[:count], refs[count:]
    rows = out_refs[0].shape[0]
    for k, out_ref in enumerate(out_refs):
        span = pl.ds(k * rows, rows)
        total = keep_ref[0, span, :] + other_ref[0, span, :].astype(jnp.float32)
        for part_ref in part_refs:
            total = total + part_ref[span, :].astype(jnp.float32)
        out_ref[...] = total.astype(jnp.bfloat16)


def total_rows_of(keep, other, parts, blocks):
    _, rows, width = keep.shape
    first = pl.BlockSpec((1, rows, width), lambda n: (0, 0, 0))
    whole = pl.BlockSpec((rows, width), lambda n: (0, 0))
    block = pl.BlockSpec((rows // blocks, width), lambda n: (0, 0))
    return pl.pallas_call(
        functools.partial(total_kernel, count=len(parts)),
        grid=(1,),
        out_shape=[jax.ShapeDtypeStruct((rows // blocks, width), jnp.bfloat16)] * blocks,
        in_specs=[first, first] + [whole] * len(parts),
        out_specs=[block] * blocks,
        compiler_params=pltpu.CompilerParams(vmem_limit_bytes=16 << 20),
        name="total_rows",
    )(keep, other, *parts)


def column_copy(source, first, width, target, sem):
    start = pl.multiple_of(first * width, LANES)
    return pltpu.make_async_copy(source.at[:, pl.ds(start, width)], target, sem)


def ids_by_row(ids_row):
    tokens = ids_row.shape[1]
    return jnp.broadcast_to(ids_row.astype(jnp.float32), (LANES, tokens)).T


def front_kernel(
    place_ref,
    table_ref,
    head_hbm,
    down_hbm,
    up_ref,
    stream_ref,
    *refs,
    owners,
    sizes,
):
    low_ref, stream_out, pick_ref, extra_ref, target_ref = refs[:5]
    up_outs = refs[5:-3]
    head_ref, down_ref, sem = refs[-3:]
    experts_ref, ids_ref = table_ref.at[0:2], table_ref.at[2:3]
    width = stream_out.shape[1]
    held_width = down_ref.shape[1]
    owner = place_ref[0]
    first_copies = [
        pltpu.make_async_copy(head_hbm, head_ref, sem.at[owners + 1]),
        pltpu.make_async_copy(down_hbm, down_ref, sem.at[owners + 2]),
    ]
    copies = [column_copy(stream_ref, owner, width, stream_out, sem.at[owners])]
    for r, out in enumerate(up_outs):
        copies.append(column_copy(up_ref, owner ^ r, width, out, sem.at[r]))
    for copy in first_copies + copies:
        copy.start()
    f32, i32 = jnp.float32, jnp.int32
    experts, halves = sizes
    tokens = ids_ref.shape[1]
    ids = ids_by_row(ids_ref[...])
    lanes = lax.broadcasted_iota(i32, (tokens, LANES), 1)
    held = held_width // ADAPTER_RANK
    lane_held = lanes - 2 * ADAPTER_RANK
    wanted = jnp.where((lane_held >= 0) & (lane_held < held), owner * held + lane_held, -1)
    tally = jnp.sum(jnp.where(ids == wanted.astype(f32), 1.0, 0.0), axis=0, keepdims=True)
    extra_ref[0:tokens, :] = jnp.where(lanes == ADAPTER_RANK, ids, 0.0)
    extra_ref[tokens : tokens + 8, :] = jnp.broadcast_to(tally, (8, LANES))

    names = lax.broadcasted_iota(i32, (experts, tokens), 0)
    hits = [experts_ref[k : k + 1, :] == names for k in range(2)]
    both = jnp.where(hits[0] | hits[1], 1.0, 0.0)
    square = (tokens, tokens)
    earlier = lax.broadcasted_iota(i32, square, 0) < lax.broadcasted_iota(i32, square, 1)
    before = jnp.dot(
        both.astype(jnp.bfloat16),
        jnp.where(earlier, 1.0, 0.0).astype(jnp.bfloat16),
        preferred_element_type=f32,
    )
    targets, chosen = [], []
    for k in range(2):
        position = jnp.sum(jnp.where(hits[k], before, 0.0), axis=0, keepdims=True).astype(i32)
        chosen.append(experts_ref[k : k + 1, :].astype(f32))
        for half in range(halves):
            slot = (experts_ref[k : k + 1, :] * halves + half) ^ place_ref[1]
            targets.append(slot * CAP + position)
    rows = lax.broadcasted_iota(i32, pick_ref.shape, 0)
    pick = functools.reduce(jnp.logical_or, [rows == target for target in targets])
    pick_ref[...] = jnp.where(pick, 1.0, 0.0).astype(jnp.bfloat16)
    filled = jnp.zeros((LANES - len(targets) - 2, tokens), f32)
    target_ref[...] = jnp.concatenate(
        chosen + [target.astype(f32) for target in targets] + [filled], axis=0
    ).T
    for copy in first_copies:
        copy.wait()
    low = jnp.dot(head_ref[...], down_ref[...], preferred_element_type=jnp.float32)
    lane = lax.broadcasted_iota(jnp.int32, (low.shape[0], LANES), 1)
    first = owner * held
    masked = []
    for start in range(0, held_width, LANES):
        adapter = (first + (lane + start) // ADAPTER_RANK).astype(jnp.float32)
        masked.append(jnp.where(ids == adapter, low[:, start : start + LANES], 0.0))
    low = jnp.concatenate(masked, axis=1).astype(jnp.bfloat16)
    fold_shape = (ADAPTER_RANK, held_width)
    fold = lax.broadcasted_iota(jnp.int32, fold_shape, 1) % ADAPTER_RANK
    fold = jnp.where(fold == lax.broadcasted_iota(jnp.int32, fold_shape, 0), 1.0, 0.0)
    low_ref[...] = lax.dot_general(
        fold.astype(jnp.bfloat16),
        low,
        (((1,), (1,)), ((), ())),
        preferred_element_type=jnp.float32,
    ).astype(jnp.bfloat16)
    for copy in copies:
        copy.wait()


def front(place, table, head_outputs, down_factors, up_factors, stream, owners, sizes):
    rows, model_width = head_outputs.shape
    total_rows = sizes[0] * sizes[1] * CAP
    width = model_width // owners
    bf16 = jnp.bfloat16
    vmem, hbm = pl.BlockSpec(memory_space=pltpu.VMEM), pl.BlockSpec(memory_space=pltpu.HBM)
    return pl.pallas_call(
        functools.partial(front_kernel, owners=owners, sizes=sizes),
        out_shape=[
            jax.ShapeDtypeStruct((ADAPTER_RANK, rows), bf16),
            jax.ShapeDtypeStruct((rows, width), bf16),
            jax.ShapeDtypeStruct((total_rows, rows), bf16),
            jax.ShapeDtypeStruct((rows + 8, LANES), jnp.float32),
            jax.ShapeDtypeStruct((rows, LANES), jnp.float32),
        ]
        + [jax.ShapeDtypeStruct((up_factors.shape[0], width), bf16)] * owners,
        in_specs=[pl.BlockSpec(memory_space=pltpu.SMEM), vmem] + [hbm] * 4,
        out_specs=[vmem] * (5 + owners),
        scratch_shapes=[
            pltpu.VMEM(head_outputs.shape, bf16),
            pltpu.VMEM(down_factors.shape, bf16),
            pltpu.SemaphoreType.DMA((owners + 3,)),
        ],
        compiler_params=pltpu.CompilerParams(vmem_limit_bytes=52 << 20),
        name="front",
    )(place, table, head_outputs, down_factors, up_factors, stream)


def route_kernel(pick_ref, extra_ref, stream_ref, *refs, owners):
    low_refs, payload_ref, out_refs = refs[:owners], refs[owners], refs[owners + 1 :]
    f32, bf16 = jnp.float32, jnp.bfloat16
    tokens, width = stream_ref.shape
    low = sum(ref[...].astype(f32) for ref in low_refs)
    lows = jnp.concatenate([low, jnp.zeros((LANES - ADAPTER_RANK, tokens), f32)], axis=0).T
    extra = extra_ref[...]
    tail = (lows + extra[:tokens]).astype(bf16)
    tally = extra[tokens : tokens + 1]
    pick = pick_ref[...]
    payload_ref[:, pl.ds(0, width)] = stream_ref[...]
    payload_ref[:, pl.ds(width, LANES)] = tail

    moved = jnp.dot(pick, stream_ref[...], preferred_element_type=f32).astype(bf16)
    moved_tail = (jnp.dot(pick, tail, preferred_element_type=f32) + tally).astype(bf16)
    for s, out_ref in enumerate(out_refs):
        out_ref[:, pl.ds(0, width)] = moved[s * CAP : (s + 1) * CAP]
        out_ref[:, pl.ds(width, LANES)] = moved_tail[s * CAP : (s + 1) * CAP]


def route(pick, extra, stream_share, low_parts, peers):
    tokens, width = stream_share.shape
    bf16 = jnp.bfloat16
    vmem = pl.BlockSpec(memory_space=pltpu.VMEM)
    return pl.pallas_call(
        functools.partial(route_kernel, owners=len(low_parts)),
        out_shape=[jax.ShapeDtypeStruct((tokens, width + LANES), bf16)]
        + [jax.ShapeDtypeStruct((CAP, width + LANES), bf16)] * peers,
        in_specs=[vmem] * (3 + len(low_parts)),
        out_specs=[vmem] * (1 + peers),
        compiler_params=pltpu.CompilerParams(vmem_limit_bytes=16 << 20),
        name="route",
    )(pick, extra, stream_share, *low_parts)


def own_kernel(payload_ref, *refs):
    up_refs = refs[:-8]
    spread_ref, adapter_ref, gain_ref, router_ref, gains_ref = refs[-8:-3]
    residual_ref, stats_ref, inverse_ref = refs[-3:]
    inverse_ref[...] = 1.0 / gains_ref[...]
    rows = payload_ref[...]
    total = with_adapter(rows, up_refs, spread_ref, adapter_ref, gain_ref.shape[1])
    residual_ref[...] = total
    scaled = (total * gain_ref[...]).astype(jnp.bfloat16)
    squares = jnp.sum(total * total, axis=1, keepdims=True)
    logits = lax.dot_general(
        router_ref[...], scaled, (((1,), (1,)), ((), ())), preferred_element_type=jnp.float32
    )
    experts = logits.shape[0]
    stats_ref[0:experts, :] = logits
    squares = jnp.broadcast_to(squares, (squares.shape[0], LANES)).T
    stats_ref[experts : 2 * experts, :] = squares[:experts]


def own_rows(payload, up_parts, spread, adapter_of, gain, router, gains):
    tokens, width = payload.shape[0], gain.shape[1]
    return pl.pallas_call(
        own_kernel,
        out_shape=[
            jax.ShapeDtypeStruct((tokens, width), jnp.float32),
            jax.ShapeDtypeStruct((2 * router.shape[0], tokens), jnp.float32),
            jax.ShapeDtypeStruct(gains.shape, jnp.float32),
        ],
        compiler_params=pltpu.CompilerParams(vmem_limit_bytes=16 << 20),
        name="own_rows",
    )(payload, *up_parts, spread, adapter_of, gain, router, gains)


def mix_kernel(target_ref, *refs, blocks, halves, model_width):
    stat_refs, block_refs = refs[: -3 - blocks], refs[-3 - blocks : -3]
    high_ref, rest_ref, load_ref = refs[-3:]
    f32 = jnp.float32
    stats = sum(ref[...] for ref in stat_refs)
    count, tokens = stats.shape
    stats = jnp.concatenate([stats, jnp.zeros((LANES - count, tokens), f32)], axis=0).T
    inv = lax.rsqrt(stats[:, count // 2 : count // 2 + 1] / model_width + EPS)
    lane = lax.broadcasted_iota(jnp.int32, stats.shape, 1).astype(f32)
    picked = [
        jnp.sum(
            jnp.where(target_ref[:, k : k + 1] == lane, stats * inv, 0.0), axis=1, keepdims=True
        )
        for k in range(2)
    ]
    slots = lax.broadcasted_iota(jnp.int32, high_ref.shape, 1).astype(f32)
    mixing = jnp.zeros(high_ref.shape, f32)
    for k in range(2):
        weight = 1.0 / (1.0 + jnp.exp(picked[1 - k] - picked[k]))
        for half in range(halves):
            column = 2 + k * halves + half
            mixing = jnp.where(slots == target_ref[:, column : column + 1], weight, mixing)
    high = mixing.astype(jnp.bfloat16)
    high_ref[...] = high
    rest_ref[...] = (mixing - high.astype(f32)).astype(jnp.bfloat16)
    load = sum(ref[...].astype(f32)[:1, :] for ref in block_refs)
    first = 2 * ADAPTER_RANK
    load_ref[...] = load[:, first : first + load_ref.shape[1]]


def mix(targets, stats, blocks, experts, model_width, held_count):
    tokens = targets.shape[0]
    peers = len(blocks)
    width = blocks[0].shape[1] - LANES
    total_rows = peers * CAP
    full = lambda shape: pl.BlockSpec(shape, lambda n: (0,) * len(shape))
    corner = pl.BlockSpec((16, LANES), lambda n: (0, width // LANES))
    return pl.pallas_call(
        functools.partial(
            mix_kernel, blocks=peers, halves=peers // experts, model_width=model_width
        ),
        grid=(1,),
        out_shape=[jax.ShapeDtypeStruct((tokens, total_rows), jnp.bfloat16)] * 2
        + [jax.ShapeDtypeStruct((1, held_count), jnp.float32)],
        in_specs=[full(targets.shape)]
        + [full(stat.shape) for stat in stats]
        + [corner] * peers,
        out_specs=[full((tokens, total_rows))] * 2 + [full((1, held_count))],
        compiler_params=pltpu.CompilerParams(vmem_limit_bytes=16 << 20),
        name="mix",
    )(targets, *stats, *blocks)


def finish_kernel(residual_ref, high_ref, rest_ref, *refs):
    block_refs, out_ref = refs[:-1], refs[-1]
    rows = jnp.concatenate([ref[...] for ref in block_refs], axis=0)
    total = jnp.dot(rest_ref[...], rows, preferred_element_type=jnp.float32)
    total = total + jnp.dot(high_ref[...], rows, preferred_element_type=jnp.float32)
    out_ref[...] = (residual_ref[...] + total).astype(out_ref.dtype)


def finish(residual, high, rest, blocks):
    return pl.pallas_call(
        finish_kernel,
        out_shape=jax.ShapeDtypeStruct(residual.shape, jnp.bfloat16),
        compiler_params=pltpu.CompilerParams(vmem_limit_bytes=16 << 20),
        name="finish",
    )(residual, high, rest, *blocks)


def shards(
    head_outputs,
    stream,
    adapter_down_factors,
    adapter_up_factors,
    norm_gain_vector,
    router_matrix,
    token_adapter_index,
    token_expert_index,
    gate_weight,
    up_weight,
    down_weight,
):
    _, model_width = head_outputs.shape
    held_width = adapter_down_factors.shape[1]
    held_count = held_width // ADAPTER_RANK
    experts = router_matrix.shape[1]
    owners = lax.axis_size("aa")
    peers = lax.axis_size("ba")
    index_aa = lax.axis_index("aa")
    index_ba = lax.axis_index("ba")
    width = model_width // owners
    f32, bf16, i32 = jnp.float32, jnp.bfloat16, jnp.int32

    place = jnp.stack([index_aa, index_ba])
    low, stream_share, pick, extra, targets, *up_parts = front(
        place,
        jnp.concatenate([token_expert_index.T, token_adapter_index[None, :]], axis=0),
        head_outputs,
        adapter_down_factors,
        adapter_up_factors,
        stream,
        owners,
        (experts, peers // experts),
    )
    low_parts = [low] + [swap(low, "aa", r) for r in range(1, owners)]
    up_parts = [up_parts[0]] + [swap(up_parts[r], "aa", r) for r in range(1, owners)]
    spots = jnp.arange(owners * held_width, dtype=i32)
    adapter_of = (index_aa ^ (spots // held_width)) * held_count + (
        spots % held_width
    ) // ADAPTER_RANK
    adapter_of = adapter_of[None, :]
    spread = (jnp.arange(ADAPTER_RANK, dtype=i32)[:, None] == spots[None, :] % ADAPTER_RANK).astype(
        bf16
    )

    payload, *outgoing = route(pick, extra, stream_share, low_parts, peers)
    near = peers // 2
    split = near + near // 2
    received = [swap(block, "ba", s) if s else block for s, block in enumerate(outgoing)]

    gain = lax.dynamic_slice_in_dim(norm_gain_vector, index_aa * width, width, 0)[None, :]
    pieces, rows_of, groups = [], [], []
    spans = ((0, near), (near, split), (split, peers))
    for first, last in spans:
        own = adapter_rows(received[first:last], up_parts, spread, adapter_of, gain)
        held = [own] + [swap(own, "aa", r) for r in range(2, owners, 2)]
        groups.append((first * CAP, (last - first) * CAP))
        for number, piece in enumerate(held):
            pieces += [piece, swap(piece, "aa", 1)]
            rows_of += [(first * CAP, 2 * number), (first * CAP, 2 * number + 1)]

    router = lax.dynamic_slice_in_dim(router_matrix.T, index_aa * width, width, 1)
    residual_share, stats, inverse = own_rows(
        payload, up_parts, spread, adapter_of, gain, router, norm_gain_vector[None, :]
    )
    stats = [stats] + [swap(stats, "aa", r) for r in range(1, owners)]
    high, rest, load = mix(
        targets, stats, received, experts, model_width, held_count
    )
    adapter_load = load.reshape(held_count)

    offsets = index_aa ^ jnp.arange(owners, dtype=i32)
    results = expert_rows(
        pieces,
        tuple(rows_of),
        tuple(groups),
        offsets,
        inverse,
        gate_weight,
        up_weight,
        down_weight,
    )

    returned = [None] * peers
    for g in (1, 2, 0):
        first, last = spans[g]
        send, keep = results[g], results[len(groups) + g]
        other = swap(send, "aa", 1)
        parts = [
            swap((keep[d] + other[d].astype(f32)).astype(bf16), "aa", 2 * d)
            for d in range(1, owners // 2)
        ]
        blocks = total_rows_of(keep, other, parts, last - first)
        for s, block in zip(range(first, last), blocks):
            returned[s] = swap(block, "ba", s) if s else block
    return (finish(residual_share, high, rest, returned), adapter_load)


def solution(mesh):
    in_specs = (
        P("ba", None),
        P("ba", None),
        P(None, "aa"),
        P("aa", None),
        P(),
        P(),
        P("ba"),
        P("ba", None),
        P("ba", None, "aa"),
        P("ba", None, "aa"),
        P("ba", "aa", None),
    )
    out_specs = (P("ba", "aa"), P("aa"))

    return jax.shard_map(shards, mesh=mesh, in_specs=in_specs, out_specs=out_specs, check_vma=False)
```
